32 devices in a mesh: section: 2 (over core), rows: 16 (over z, y, x).
Axes of the slice: x: 2, y: 2, z: 4, core: 2. Of those that a mesh axis runs over, the one named last changes fastest.
Arguments:
- table: float32 [16384, 64], P('rows', 'section'), may hold values from -6 to 6
- mask: int32 [16384], P('rows'), may hold values from 0 to 1, as said below
- weight: float32 [64, 1024], replicated, may hold values from -0.75 to 0.75
- bias: float32 [1024], replicated, may hold values from -3 to 3
Outputs:
- projected: bfloat16 [16384, 1024], P('rows', 'section')
The draws below stay inside these ranges and needn't reach their ends.
Inputs may be any that keep to these rules, and one draw needn't show every extreme that they name: `mask`: the probability that a row survives is constant within one device's rows and drawn afresh for each device, from about 5 to 95 percent.
All inputs are finite; a program needn't handle non-finite values.
Results may differ from the reference program's by a relative error of at most 0.001.
Values sent between devices are 32-bit elements; how exact they have to be, the bound alone decides.
A program may use at most 64 MiB of HBM per device.

```python
import jax
import jax.numpy as jnp
from jax import lax

C = 64
F = 1024
ROWS_DEV = 1024
TOTAL = 16384
N_ROWS = 16


def draw_mask(key, part):
    blocks = TOTAL // ROWS_DEV
    first, second = jax.random.split(jax.random.fold_in(key, 11))
    rates = jax.random.randint(first, (blocks,), 50, 950)
    levels = jnp.repeat(rates, ROWS_DEV)
    ticket = jax.random.randint(second, (TOTAL,), 0, 1000)
    return (ticket < levels).astype(jnp.int32)


def block_levels(key, extent, cuts, smallest, largest):
    factor_of, own = 1.0, jax.random.fold_in(key, 6)
    for axis_at, parts in cuts:
        draws = jnp.exp(jax.random.uniform(jax.random.fold_in(own, axis_at), (parts,), jnp.float32, smallest / len(cuts), largest / len(cuts)))
        factor_of = factor_of * jnp.repeat(draws, extent[axis_at] // parts).reshape([-1 if axis == axis_at else 1 for axis in range(len(extent))])
    return factor_of


def noise(rng, dims, scale, limit, shards=(), kind=jnp.bfloat16):
    gain = block_levels(rng, dims, shards, -0.22, 0.18) if shards else 1.0
    array = jax.random.normal(rng, dims, jnp.float32) * scale * gain
    return jnp.minimum(jnp.maximum(array, -limit), limit).astype(kind)


def setup_inputs(seed: int = 0) -> dict:
    key_of = jax.random.split(jax.random.key(seed), 5)
    table = noise(key_of[0], (TOTAL, C), 1.0, 6.0, ((0, 16), (1, 2)), jnp.float32)
    mask = draw_mask(jax.random.fold_in(key_of[4], 71), 0)
    weight = noise(key_of[2], (C, F), C ** -0.5, 0.75, (), jnp.float32)
    bias = noise(key_of[3], (F,), 0.5, 3.0, (), jnp.float32)
    return dict(table=table, mask=mask, weight=weight, bias=bias)


def reference(table, mask, weight, bias):
    rank = (jnp.cumsum(mask) - mask).astype(jnp.int32)
    total = jnp.sum(mask).astype(jnp.int32)
    place = jnp.where(mask == 1, rank, TOTAL).astype(jnp.int32)
    packed = jnp.zeros((TOTAL, C), jnp.float32).at[place].set(table, mode="drop")
    blocks = packed.reshape(N_ROWS, ROWS_DEV, C)
    starts = jnp.arange(N_ROWS, dtype=jnp.int32)

    def project(args):
        block, start = args
        result = jnp.dot(block, weight, precision=lax.Precision.HIGHEST, preferred_element_type=jnp.float32) + bias
        filled = start * ROWS_DEV + jnp.arange(ROWS_DEV, dtype=jnp.int32) < total
        return jnp.where(filled[:, None], result, 0.0).astype(jnp.bfloat16)

    projected = lax.map(project, (blocks, starts))
    return projected.reshape(TOTAL, F)
```

```python
import functools

import jax
import jax.numpy as jnp
from jax import lax
from jax.experimental import pallas as pl
from jax.experimental.pallas import tpu as pltpu
from jax.sharding import PartitionSpec as P

CHUNKS = 4
F32 = jnp.float32
BF16 = jnp.bfloat16
I32 = jnp.int32


def split(x, terms):
    parts = []
    for _ in range(terms):
        part = x.astype(BF16)
        parts.append(part)
        x = x - part.astype(F32)
    return parts


def kernel(
    n, table_ref, mask_ref, w_ref, bias_ref, out_ref,
    counts, prefix, hold, came, joined, wcat, send_sem, recv_sem, count_send, count_recv,
):
    height, half = table_ref.shape
    cols, width = w_ref.shape[0], out_ref.shape[1]
    lines = height // 128
    levels = (n - 1).bit_length()
    lanes = height // CHUNKS
    me = lax.axis_index("rows")
    core = lax.axis_index("section")

    barrier = pltpu.get_barrier_semaphore()

    def greet(step, carry):
        pl.semaphore_signal(barrier, inc=1, device_id={"rows": lax.rem(me + step, n)})
        return carry

    lax.fori_loop(1, n, greet, 0)
    pl.semaphore_signal(barrier, inc=1, device_id={"section": 1 - core})

    mask = mask_ref[...]
    ones = mask.astype(F32).astype(BF16)
    row = lax.broadcasted_iota(I32, (128, 128), 0)
    col = lax.broadcasted_iota(I32, (128, 128), 1)
    before = jnp.where(row < col, 1.0, 0.0).astype(BF16)
    inner = jnp.dot(ones, before, preferred_element_type=F32).astype(I32)
    sums = jnp.dot(ones, jnp.ones((128, 128), BF16), preferred_element_type=F32).astype(I32)
    running = jnp.zeros((1, 128), I32)
    starts = []
    for line in range(lines):
        starts.append(running)
        running = running + sums[line : line + 1]
    rank = inner + jnp.concatenate(starts, 0)
    counts[me] = running

    pl.semaphore_wait(barrier, n)

    def count_copy(step):
        peer = lax.rem(me + step, n)
        return pltpu.make_async_remote_copy(
            src_ref=counts.at[me], dst_ref=counts.at[me],
            send_sem=count_send.at[step], recv_sem=count_recv.at[step],
            device_id={"rows": peer},
        )

    def count_start(step, carry):
        count_copy(step).start()
        return carry

    def count_wait(step, carry):
        count_copy(step).wait()
        return carry

    lax.fori_loop(1, n, count_start, 0)

    w = w_ref[:, pl.ds(pl.multiple_of(core * width, 128), width)]
    bias = bias_ref[:, pl.ds(pl.multiple_of(core * width, 128), width)]
    w_hi, w_lo = split(w, 2)
    b_hi, b_mid, b_lo = [part.astype(F32) for part in split(bias, 3)]
    line = lax.broadcasted_iota(I32, (16, width), 0)
    extra = jnp.where(line == 0, b_hi, jnp.where(line == 1, b_mid, jnp.where(line == 2, b_lo, 0.0)))
    wcat[...] = jnp.concatenate([w_hi, w_lo, w_hi, extra.astype(BF16)], 0)
    turned = jnp.concatenate(split(table_ref[...].T, 3), 0)

    lax.fori_loop(1, n, count_wait, 0)
    total = jnp.zeros((1, 128), I32)
    for device in range(n):
        prefix[device] = total
        total = total + counts[device]
    prefix[n] = total

    slot = jnp.where(mask == 1, (rank + prefix[me]) & (height - 1), -1)

    def wide(x):
        return jnp.concatenate([x] * (lanes // 128), 1)

    def data_copy(level, chunk):
        at = (slice(None), pl.ds(chunk * lanes, lanes))
        return pltpu.make_async_remote_copy(
            src_ref=hold.at[(level,) + at], dst_ref=came.at[(level,) + at],
            send_sem=send_sem.at[level, chunk], recv_sem=recv_sem.at[level, chunk],
            device_id={"rows": me + (1 - 2 * (me // (1 << level) % 2)) * (1 << level)},
        )

    def join_copy(chunk):
        at = (core, slice(None), pl.ds(chunk * lanes, lanes))
        return pltpu.make_async_remote_copy(
            src_ref=joined.at[at], dst_ref=joined.at[at],
            send_sem=send_sem.at[levels, chunk], recv_sem=recv_sem.at[levels, chunk],
            device_id={"section": 1 - core},
        )

    for chunk in range(CHUNKS):
        here = chunk * lanes + lax.broadcasted_iota(I32, (lanes, 128), 0)
        hot = jnp.concatenate(
            [jnp.where(here == slot[b : b + 1], 1.0, 0.0).astype(BF16) for b in range(lines)], 1
        )
        folded = lax.dot_general(
            turned, hot, (((1,), (1,)), ((), ())), preferred_element_type=F32
        )
        hold[0, :, chunk * lanes : (chunk + 1) * lanes] = (
            folded[:half] + folded[half : 2 * half]
        ) + folded[2 * half :]
        data_copy(0, chunk).start()

    for level in range(levels):
        reach = 2 << level
        group = me // reach * reach
        bit = me // (1 << level) % 2
        low = wide(prefix[group])
        middle = wide(prefix[group + (1 << level)])
        for chunk in range(CHUNKS):
            at = slice(chunk * lanes, (chunk + 1) * lanes)
            data_copy(level, chunk).wait_recv()
            base = (me % reach) * height + chunk * lanes
            base = base + lax.broadcasted_iota(I32, (1, lanes), 1)
            place = low + ((base - low) & (reach * height - 1))
            upper = jnp.where(place >= middle, 1, 0)
            foreign = jnp.broadcast_to(upper, (half, lanes)) != bit
            block = jnp.where(foreign, came[level, :, at], hold[level, :, at])
            if level < levels - 1:
                hold[level + 1, :, at] = block
                data_copy(level + 1, chunk).start()
            else:
                joined[core, :, at] = block
                join_copy(chunk).start()

    ends = wide(total)
    for chunk in range(CHUNKS):
        at = slice(chunk * lanes, (chunk + 1) * lanes)
        join_copy(chunk).wait_recv()
        own = me * height + chunk * lanes + lax.broadcasted_iota(I32, (1, lanes), 1)
        filled = jnp.where(own < ends, 1.0, 0.0)
        rows = jnp.concatenate([joined[0, :, at], joined[1, :, at]], 0)
        rows = jnp.where(jnp.broadcast_to(filled, rows.shape) > 0.5, rows, 0.0)
        a_hi, a_lo = split(rows, 2)
        marks = jnp.broadcast_to(filled, (16, lanes)).astype(BF16)
        lhs = jnp.concatenate([a_hi, a_hi, a_lo, marks], 0)
        out_ref[at, :] = lax.dot_general(
            lhs, wcat[...], (((0,), (0,)), ((), ())), preferred_element_type=F32
        ).astype(BF16)

    for level in range(levels):
        for chunk in range(CHUNKS):
            data_copy(level, chunk).wait_send()
    for chunk in range(CHUNKS):
        join_copy(chunk).wait_send()


def solution(mesh):
    n, sections = mesh.shape["rows"], mesh.shape["section"]

    def step(table, mask, weight, bias):
        height, half = table.shape
        cols, features = weight.shape
        width = features // sections
        levels = (n - 1).bit_length()
        return pl.pallas_call(
            functools.partial(kernel, n),
            name="filter_project",
            out_shape=jax.ShapeDtypeStruct((height, width), BF16),
            in_specs=[pl.BlockSpec(memory_space=pltpu.VMEM)] * 4,
            out_specs=pl.BlockSpec(memory_space=pltpu.VMEM),
            scratch_shapes=[
                pltpu.VMEM((n, 1, 128), I32),
                pltpu.VMEM((n + 1, 1, 128), I32),
                pltpu.VMEM((levels, half, height), F32),
                pltpu.VMEM((levels, half, height), F32),
                pltpu.VMEM((sections, half, height), F32),
                pltpu.VMEM((3 * cols + 16, width), BF16),
                pltpu.SemaphoreType.DMA((levels + 1, CHUNKS)),
                pltpu.SemaphoreType.DMA((levels + 1, CHUNKS)),
                pltpu.SemaphoreType.DMA((n,)),
                pltpu.SemaphoreType.DMA((n,)),
            ],
            compiler_params=pltpu.CompilerParams(collective_id=0, has_side_effects=True),
        )(table, mask.reshape(height // 128, 128), weight, bias.reshape(1, features))

    return jax.shard_map(
        step,
        mesh=mesh,
        in_specs=(P("rows", "section"), P("rows"), P(), P()),
        out_specs=P("rows", "section"),
        check_vma=False,
    )
```

```python
import functools

import jax
import jax.numpy as jnp
from jax import lax
from jax.experimental import pallas as pl
from jax.experimental.pallas import tpu as pltpu
from jax.sharding import PartitionSpec as P

CHUNKS = 4
PLANE = 4
RAW = 4
F32 = jnp.float32
BF16 = jnp.bfloat16
I32 = jnp.int32


def split(x, terms):
    parts = []
    for _ in range(terms):
        part = x.astype(BF16)
        parts.append(part)
        x = x - part.astype(F32)
    return parts


def kernel(
    n, table_hbm, mask_hbm, w_hbm, bias_hbm, out_ref,
    table_ref, mask_ref, bias_ref,
    tally, planes, prefix, raw, hold, came, joined, w_ref, wcat,
    send_sem, recv_sem, raw_send, raw_recv, count_send, count_recv, plane_send, plane_recv, load_sem,
):
    half, height = table_hbm.shape
    width = out_ref.shape[1]
    lines = height // 128
    levels = (n - 1).bit_length()
    lanes = height // CHUNKS
    side = min(PLANE, n)
    crowd = min(RAW, n)
    first = (crowd - 1).bit_length()
    count_planes = n // side
    me = lax.axis_index("rows")
    core = lax.axis_index("section")
    plane = me // side
    seat = lax.rem(me, side)

    columns = pl.ds(pl.multiple_of(core * width, 128), width)
    mask_copy = pltpu.make_async_copy(mask_hbm, mask_ref, load_sem.at[0])
    table_copy = pltpu.make_async_copy(table_hbm, table_ref, load_sem.at[1])
    w_copy = pltpu.make_async_copy(w_hbm.at[:, columns], w_ref, load_sem.at[2])
    bias_copy = pltpu.make_async_copy(bias_hbm.at[:, columns], bias_ref, load_sem.at[3])
    for load in (mask_copy, table_copy, w_copy, bias_copy):
        load.start()

    def seat_peer(step):
        return plane * side + lax.rem(seat + step, side)

    def plane_peer(step):
        return lax.rem(plane + step, count_planes) * side + seat

    barrier = pltpu.get_barrier_semaphore()
    for step in range(1, side):
        pl.semaphore_signal(barrier, inc=1, device_id={"rows": seat_peer(step)})
    for step in range(1, count_planes):
        pl.semaphore_signal(barrier, inc=1, device_id={"rows": plane_peer(step)})
    pl.semaphore_signal(barrier, inc=1, device_id={"section": 1 - core})

    mask_copy.wait()
    mask = mask_ref[...]
    ones = mask.astype(F32).astype(BF16)
    row = lax.broadcasted_iota(I32, (128, 128), 0)
    col = lax.broadcasted_iota(I32, (128, 128), 1)
    before = jnp.where(row < col, 1.0, 0.0).astype(BF16)
    inner = jnp.dot(ones, before, preferred_element_type=F32).astype(I32)
    sums = jnp.dot(ones, jnp.ones((128, 128), BF16), preferred_element_type=F32).astype(I32)
    running = jnp.zeros((1, 128), I32)
    starts = []
    for line in range(lines):
        starts.append(running)
        running = running + sums[line : line + 1]
    tally[seat] = running
    slot = jnp.where(mask == 1, inner + jnp.concatenate(starts, 0), -1)

    own = lax.rem(me, crowd)
    table_copy.wait()
    turned = jnp.concatenate(split(table_ref[...], 3), 0)
    for chunk in range(CHUNKS):
        here = chunk * lanes + lax.broadcasted_iota(I32, (lanes, 128), 0)
        hot = jnp.concatenate(
            [jnp.where(here == slot[b : b + 1], 1.0, 0.0).astype(BF16) for b in range(lines)], 1
        )
        folded = lax.dot_general(
            turned, hot, (((1,), (1,)), ((), ())), preferred_element_type=F32
        )
        raw[own, :, chunk * lanes : (chunk + 1) * lanes] = (
            folded[:half] + folded[half : 2 * half]
        ) + folded[2 * half :]

    pl.semaphore_wait(barrier, side + count_planes - 1)

    def seat_copy(step):
        return pltpu.make_async_remote_copy(
            src_ref=tally.at[seat], dst_ref=tally.at[seat],
            send_sem=count_send.at[step], recv_sem=count_recv.at[step],
            device_id={"rows": seat_peer(step)},
        )

    def plane_copy(step):
        return pltpu.make_async_remote_copy(
            src_ref=planes.at[plane], dst_ref=planes.at[plane],
            send_sem=plane_send.at[step], recv_sem=plane_recv.at[step],
            device_id={"rows": plane_peer(step)},
        )

    def raw_copy(step):
        return pltpu.make_async_remote_copy(
            src_ref=raw.at[own], dst_ref=raw.at[own],
            send_sem=raw_send.at[step], recv_sem=raw_recv.at[step],
            device_id={"rows": me - own + lax.rem(own + step, crowd)},
        )

    for step in range(1, side):
        seat_copy(step).start()
    for step in range(1, crowd):
        raw_copy(step).start()
    for step in range(1, side):
        seat_copy(step).wait_recv()
    everyone = jnp.zeros((1, 128), I32)
    for at in range(side):
        everyone = everyone + tally[at]
    planes[plane] = everyone
    for step in range(1, count_planes):
        plane_copy(step).start()

    w_copy.wait()
    bias_copy.wait()
    bias = bias_ref[...]
    w_hi, w_lo = split(w_ref[...], 2)
    b_hi, b_mid, b_lo = [part.astype(F32) for part in split(bias, 3)]
    line = lax.broadcasted_iota(I32, (16, width), 0)
    extra = jnp.where(line == 0, b_hi, jnp.where(line == 1, b_mid, jnp.where(line == 2, b_lo, 0.0)))
    wcat[...] = jnp.concatenate([w_hi, w_lo, w_hi, extra.astype(BF16)], 0)

    for step in range(1, count_planes):
        plane_copy(step).wait_recv()
    total = jnp.zeros((1, 128), I32)
    for at in range(count_planes):
        prefix[at * side] = total
        total = total + planes[at]
    prefix[n] = total
    running = prefix[plane * side]
    for at in range(side - 1):
        running = running + tally[at]
        prefix[plane * side + at + 1] = running

    def wide(x):
        return jnp.concatenate([x] * (lanes // 128), 1)

    def data_copy(level, chunk):
        at = (slice(None), pl.ds(chunk * lanes, lanes))
        return pltpu.make_async_remote_copy(
            src_ref=hold.at[(level,) + at], dst_ref=came.at[(level,) + at],
            send_sem=send_sem.at[level, chunk], recv_sem=recv_sem.at[level, chunk],
            device_id={"rows": me + (1 - 2 * (me // (1 << level) % 2)) * (1 << level)},
        )

    def join_copy(chunk):
        at = (core, slice(None), pl.ds(chunk * lanes, lanes))
        return pltpu.make_async_remote_copy(
            src_ref=joined.at[at], dst_ref=joined.at[at],
            send_sem=send_sem.at[levels, chunk], recv_sem=recv_sem.at[levels, chunk],
            device_id={"section": 1 - core},
        )

    for step in range(1, crowd):
        raw_copy(step).wait_recv()
    turns = []
    for at in range(crowd):
        shift = (prefix[me - own + at] & (height - 1))[0, 0]
        turns.append(pltpu.roll(raw[at], shift, 1))
    low = wide(prefix[me - own])
    for chunk in range(CHUNKS):
        at = slice(chunk * lanes, (chunk + 1) * lanes)
        base = own * height + chunk * lanes + lax.broadcasted_iota(I32, (1, lanes), 1)
        place = low + ((base - low) & (crowd * height - 1))
        place = jnp.broadcast_to(place, (half, lanes))
        block = turns[0][:, at]
        for other in range(1, crowd):
            block = jnp.where(place >= wide(prefix[me - own + other]), turns[other][:, at], block)
        hold[first, :, at] = block
        data_copy(first, chunk).start()

    for level in range(first, levels):
        reach = 2 << level
        group = me // reach * reach
        bit = me // (1 << level) % 2
        low = wide(prefix[group])
        middle = wide(prefix[group + (1 << level)])
        for chunk in range(CHUNKS):
            at = slice(chunk * lanes, (chunk + 1) * lanes)
            data_copy(level, chunk).wait_recv()
            base = (me % reach) * height + chunk * lanes
            base = base + lax.broadcasted_iota(I32, (1, lanes), 1)
            place = low + ((base - low) & (reach * height - 1))
            upper = jnp.where(place >= middle, 1, 0)
            foreign = jnp.broadcast_to(upper, (half, lanes)) != bit
            block = jnp.where(foreign, came[level, :, at], hold[level, :, at])
            if level < levels - 1:
                hold[level + 1, :, at] = block
                data_copy(level + 1, chunk).start()
            else:
                joined[core, :, at] = block
                join_copy(chunk).start()

    ends = wide(total)
    for chunk in range(CHUNKS):
        at = slice(chunk * lanes, (chunk + 1) * lanes)
        join_copy(chunk).wait_recv()
        owned = me * height + chunk * lanes + lax.broadcasted_iota(I32, (1, lanes), 1)
        filled = jnp.where(owned < ends, 1.0, 0.0)
        rows = jnp.concatenate([joined[0, :, at], joined[1, :, at]], 0)
        rows = jnp.where(jnp.broadcast_to(filled, rows.shape) > 0.5, rows, 0.0)
        a_hi, a_lo = split(rows, 2)
        marks = jnp.broadcast_to(filled, (16, lanes)).astype(BF16)
        lhs = jnp.concatenate([a_hi, a_hi, a_lo, marks], 0)
        out_ref[at, :] = lax.dot_general(
            lhs, wcat[...], (((0,), (0,)), ((), ())), preferred_element_type=F32
        ).astype(BF16)

    for step in range(1, side):
        seat_copy(step).wait_send()
    for step in range(1, count_planes):
        plane_copy(step).wait_send()
    for step in range(1, crowd):
        raw_copy(step).wait_send()
    for level in range(first, levels):
        for chunk in range(CHUNKS):
            data_copy(level, chunk).wait_send()
    for chunk in range(CHUNKS):
        join_copy(chunk).wait_send()


def solution(mesh):
    n, sections = mesh.shape["rows"], mesh.shape["section"]

    def step(table, mask, weight, bias):
        height, half = table.shape
        cols, features = weight.shape
        width = features // sections
        levels = (n - 1).bit_length()
        side, crowd = min(PLANE, n), min(RAW, n)
        vmem = pl.BlockSpec(memory_space=pltpu.VMEM)
        sem = pltpu.SemaphoreType.DMA
        return pl.pallas_call(
            functools.partial(kernel, n),
            name="filter_project",
            out_shape=jax.ShapeDtypeStruct((height, width), BF16),
            in_specs=[pl.BlockSpec(memory_space=pltpu.HBM)] * 4,
            out_specs=vmem,
            scratch_shapes=[
                pltpu.VMEM((half, height), F32),
                pltpu.VMEM((height // 128, 128), I32),
                pltpu.VMEM((1, width), F32),
                pltpu.VMEM((side, 1, 128), I32),
                pltpu.VMEM((n // side, 1, 128), I32),
                pltpu.VMEM((n + 1, 1, 128), I32),
                pltpu.VMEM((crowd, half, height), F32),
                pltpu.VMEM((levels, half, height), F32),
                pltpu.VMEM((levels, half, height), F32),
                pltpu.VMEM((sections, half, height), F32),
                pltpu.VMEM((cols, width), F32),
                pltpu.VMEM((3 * cols + 16, width), BF16),
                sem((levels + 1, CHUNKS)), sem((levels + 1, CHUNKS)),
                sem((crowd,)), sem((crowd,)),
                sem((side,)), sem((side,)),
                sem((n // side,)), sem((n // side,)),
                sem((4,)),
            ],
            compiler_params=pltpu.CompilerParams(
                collective_id=0, has_side_effects=True, vmem_limit_bytes=16 << 20
            ),
        )(table.T, mask.reshape(height // 128, 128), weight, bias.reshape(1, features))

    return jax.shard_map(
        step,
        mesh=mesh,
        in_specs=(P("rows", "section"), P("rows"), P(), P()),
        out_specs=P("rows", "section"),
        check_vma=False,
    )
```

```python
import functools

import jax
import jax.numpy as jnp
from jax import lax
from jax.experimental import pallas as pl
from jax.experimental.pallas import tpu as pltpu
from jax.sharding import PartitionSpec as P

CHUNKS = 4
PLANE = 4
RAW = 4
F32 = jnp.float32
BF16 = jnp.bfloat16
I32 = jnp.int32


def split(x, terms):
    parts = []
    for _ in range(terms):
        part = x.astype(BF16)
        parts.append(part)
        x = x - part.astype(F32)
    return parts


def kernel(
    n, table_hbm, mask_hbm, w_hbm, bias_hbm, out_ref,
    table_ref, mask_ref, bias_ref,
    tally, planes, prefix, raw, hold, came, joined, w_ref, wcat,
    send_sem, recv_sem, raw_send, raw_recv, count_send, count_recv, plane_send, plane_recv, load_sem,
):
    half, height = table_hbm.shape
    width = out_ref.shape[1]
    lines = height // 128
    levels = (n - 1).bit_length()
    lanes = height // CHUNKS
    side = min(PLANE, n)
    crowd = min(RAW, n)
    first = (crowd - 1).bit_length()
    count_planes = n // side
    me = lax.axis_index("rows")
    core = lax.axis_index("section")
    plane = me // side
    seat = lax.rem(me, side)

    columns = pl.ds(pl.multiple_of(core * width, 128), width)
    mask_copy = pltpu.make_async_copy(mask_hbm, mask_ref, load_sem.at[0])
    table_copy = pltpu.make_async_copy(table_hbm, table_ref, load_sem.at[1])
    w_copy = pltpu.make_async_copy(w_hbm.at[:, columns], w_ref, load_sem.at[2])
    bias_copy = pltpu.make_async_copy(bias_hbm.at[:, columns], bias_ref, load_sem.at[3])
    for load in (mask_copy, table_copy, w_copy, bias_copy):
        load.start()

    def seat_peer(step):
        return plane * side + lax.rem(seat + step, side)

    def plane_peer(step):
        return lax.rem(plane + step, count_planes) * side + seat

    barrier = pltpu.get_barrier_semaphore()
    for step in range(1, side):
        pl.semaphore_signal(barrier, inc=1, device_id={"rows": seat_peer(step)})
    for step in range(1, count_planes):
        pl.semaphore_signal(barrier, inc=1, device_id={"rows": plane_peer(step)})
    pl.semaphore_signal(barrier, inc=1, device_id={"section": 1 - core})

    mask_copy.wait()
    mask = mask_ref[...]
    ones = mask.astype(F32).astype(BF16)
    row = lax.broadcasted_iota(I32, (128, 128), 0)
    col = lax.broadcasted_iota(I32, (128, 128), 1)
    before = jnp.where(row < col, 1.0, 0.0).astype(BF16)
    inner = jnp.dot(ones, before, preferred_element_type=F32).astype(I32)
    sums = jnp.dot(ones, jnp.ones((128, 128), BF16), preferred_element_type=F32).astype(I32)
    running = jnp.zeros((1, 128), I32)
    starts = []
    for line in range(lines):
        starts.append(running)
        running = running + sums[line : line + 1]
    tally[seat] = running
    slot = jnp.where(mask == 1, inner + jnp.concatenate(starts, 0), -1)

    own = lax.rem(me, crowd)
    table_copy.wait()
    turned = jnp.concatenate(split(table_ref[...], 3), 0)
    for chunk in range(CHUNKS):
        here = chunk * lanes + lax.broadcasted_iota(I32, (lanes, 128), 0)
        hot = jnp.concatenate(
            [jnp.where(here == slot[b : b + 1], 1.0, 0.0).astype(BF16) for b in range(lines)], 1
        )
        folded = lax.dot_general(
            turned, hot, (((1,), (1,)), ((), ())), preferred_element_type=F32
        )
        raw[own, :, chunk * lanes : (chunk + 1) * lanes] = (
            folded[:half] + folded[half : 2 * half]
        ) + folded[2 * half :]

    pl.semaphore_wait(barrier, side + count_planes - 1)

    def seat_copy(step):
        return pltpu.make_async_remote_copy(
            src_ref=tally.at[seat], dst_ref=tally.at[seat],
            send_sem=count_send.at[step], recv_sem=count_recv.at[step],
            device_id={"rows": seat_peer(step)},
        )

    def plane_copy(step):
        return pltpu.make_async_remote_copy(
            src_ref=planes.at[plane], dst_ref=planes.at[plane],
            send_sem=plane_send.at[step], recv_sem=plane_recv.at[step],
            device_id={"rows": plane_peer(step)},
        )

    def raw_copy(step):
        return pltpu.make_async_remote_copy(
            src_ref=raw.at[own], dst_ref=raw.at[own],
            send_sem=raw_send.at[step], recv_sem=raw_recv.at[step],
            device_id={"rows": me - own + lax.rem(own + step, crowd)},
        )

    for step in range(1, side):
        seat_copy(step).start()
    for step in range(1, crowd):
        raw_copy(step).start()
    for step in range(1, side):
        seat_copy(step).wait_recv()
    everyone = jnp.zeros((1, 128), I32)
    for at in range(side):
        everyone = everyone + tally[at]
    planes[plane] = everyone
    for step in range(1, count_planes):
        plane_copy(step).start()

    w_copy.wait()
    bias_copy.wait()
    bias = bias_ref[...]
    w_hi, w_lo = split(w_ref[...], 2)
    b_hi, b_mid, b_lo = [part.astype(F32) for part in split(bias, 3)]
    line = lax.broadcasted_iota(I32, (16, width), 0)
    extra = jnp.where(line == 0, b_hi, jnp.where(line == 1, b_mid, jnp.where(line == 2, b_lo, 0.0)))
    wcat[...] = jnp.concatenate([w_hi, w_lo, w_hi, extra.astype(BF16)], 0)

    for step in range(1, count_planes):
        plane_copy(step).wait_recv()
    total = jnp.zeros((1, 128), I32)
    for at in range(count_planes):
        prefix[at * side] = total
        total = total + planes[at]
    prefix[n] = total
    running = prefix[plane * side]
    for at in range(side - 1):
        running = running + tally[at]
        prefix[plane * side + at + 1] = running

    def wide(x):
        return jnp.concatenate([x] * (lanes // 128), 1)

    def data_copy(level, chunk):
        at = (slice(None), pl.ds(chunk * lanes, lanes))
        return pltpu.make_async_remote_copy(
            src_ref=hold.at[(level,) + at], dst_ref=came.at[(level,) + at],
            send_sem=send_sem.at[level, chunk], recv_sem=recv_sem.at[level, chunk],
            device_id={"rows": me + (1 - 2 * (me // (1 << level) % 2)) * (1 << level)},
        )

    def join_copy(chunk):
        at = (core, slice(None), pl.ds(chunk * lanes, lanes))
        return pltpu.make_async_remote_copy(
            src_ref=joined.at[at], dst_ref=joined.at[at],
            send_sem=send_sem.at[levels, chunk], recv_sem=recv_sem.at[levels, chunk],
            device_id={"section": 1 - core},
        )

    for step in range(1, crowd):
        raw_copy(step).wait_recv()
    turns = []
    for at in range(crowd):
        shift = (prefix[me - own + at] & (height - 1))[0, 0]
        turns.append(pltpu.roll(raw[at], shift, 1))
    low = wide(prefix[me - own])
    for chunk in range(CHUNKS):
        at = slice(chunk * lanes, (chunk + 1) * lanes)
        base = own * height + chunk * lanes + lax.broadcasted_iota(I32, (1, lanes), 1)
        place = low + ((base - low) & (crowd * height - 1))
        place = jnp.broadcast_to(place, (half, lanes))
        block = turns[0][:, at]
        for other in range(1, crowd):
            block = jnp.where(place >= wide(prefix[me - own + other]), turns[other][:, at], block)
        hold[first, :, at] = block
        data_copy(first, chunk).start()

    for level in range(first, levels):
        reach = 2 << level
        group = me // reach * reach
        bit = me // (1 << level) % 2
        low = wide(prefix[group])
        middle = wide(prefix[group + (1 << level)])
        for chunk in range(CHUNKS):
            at = slice(chunk * lanes, (chunk + 1) * lanes)
            data_copy(level, chunk).wait_recv()
            base = (me % reach) * height + chunk * lanes
            base = base + lax.broadcasted_iota(I32, (1, lanes), 1)
            place = low + ((base - low) & (reach * height - 1))
            upper = jnp.where(place >= middle, 1, 0)
            foreign = jnp.broadcast_to(upper, (half, lanes)) != bit
            block = jnp.where(foreign, came[level, :, at], hold[level, :, at])
            if level < levels - 1:
                hold[level + 1, :, at] = block
                data_copy(level + 1, chunk).start()
            else:
                joined[core, :, at] = block
                join_copy(chunk).start()

    ends = wide(total)
    for chunk in range(CHUNKS):
        at = slice(chunk * lanes, (chunk + 1) * lanes)
        join_copy(chunk).wait_recv()
        owned = me * height + chunk * lanes + lax.broadcasted_iota(I32, (1, lanes), 1)
        filled = jnp.where(owned < ends, 1.0, 0.0)
        rows = jnp.concatenate([joined[0, :, at], joined[1, :, at]], 0)
        rows = jnp.where(jnp.broadcast_to(filled, rows.shape) > 0.5, rows, 0.0)
        a_hi, a_lo = split(rows, 2)
        marks = jnp.broadcast_to(filled, (16, lanes)).astype(BF16)
        lhs = jnp.concatenate([a_hi, a_hi, a_lo, marks], 0)
        out_ref[at, :] = lax.dot_general(
            lhs, wcat[...], (((0,), (0,)), ((), ())), preferred_element_type=F32
        ).astype(BF16)

    for step in range(1, side):
        seat_copy(step).wait_send()
    for step in range(1, count_planes):
        plane_copy(step).wait_send()
    for step in range(1, crowd):
        raw_copy(step).wait_send()
    for level in range(first, levels):
        for chunk in range(CHUNKS):
            data_copy(level, chunk).wait_send()
    for chunk in range(CHUNKS):
        join_copy(chunk).wait_send()


def solution(mesh):
    n, sections = mesh.shape["rows"], mesh.shape["section"]

    def step(table, mask, weight, bias):
        height, half = table.shape
        cols, features = weight.shape
        width = features // sections
        levels = (n - 1).bit_length()
        side, crowd = min(PLANE, n), min(RAW, n)
        operands = table.T, mask.reshape(height // 128, 128), weight, bias.reshape(1, features)
        vmem = pl.BlockSpec(memory_space=pltpu.VMEM)
        sem = pltpu.SemaphoreType.DMA
        return pl.pallas_call(
            functools.partial(kernel, n),
            name="filter_project",
            out_shape=jax.ShapeDtypeStruct((height, width), BF16),
            in_specs=[pl.BlockSpec(memory_space=pltpu.HBM)] * 4,
            out_specs=vmem,
            scratch_shapes=[
                pltpu.VMEM((half, height), F32),
                pltpu.VMEM((height // 128, 128), I32),
                pltpu.VMEM((1, width), F32),
                pltpu.VMEM((side, 1, 128), I32),
                pltpu.VMEM((n // side, 1, 128), I32),
                pltpu.VMEM((n + 1, 1, 128), I32),
                pltpu.VMEM((crowd, half, height), F32),
                pltpu.VMEM((levels, half, height), F32),
                pltpu.VMEM((levels, half, height), F32),
                pltpu.VMEM((sections, half, height), F32),
                pltpu.VMEM((cols, width), F32),
                pltpu.VMEM((3 * cols + 16, width), BF16),
                sem((levels + 1, CHUNKS)), sem((levels + 1, CHUNKS)),
                sem((crowd,)), sem((crowd,)),
                sem((side,)), sem((side,)),
                sem((n // side,)), sem((n // side,)),
                sem((4,)),
            ],
            compiler_params=pltpu.CompilerParams(
                collective_id=0, has_side_effects=True, vmem_limit_bytes=16 << 20
            ),
        )(*[pltpu.with_memory_space_constraint(x, pltpu.HBM) for x in operands])

    return jax.shard_map(
        step,
        mesh=mesh,
        in_specs=(P("rows", "section"), P("rows"), P(), P()),
        out_specs=P("rows", "section"),
        check_vma=False,
    )
```

```python
import functools

import jax
import jax.numpy as jnp
from jax import lax
from jax.experimental import pallas as pl
from jax.experimental.pallas import tpu as pltpu
from jax.sharding import PartitionSpec as P

CHUNKS = 4
PLANE = 4
RAW = 4
F32 = jnp.float32
BF16 = jnp.bfloat16
I32 = jnp.int32


def split(x, terms):
    parts = []
    for _ in range(terms):
        part = x.astype(BF16)
        parts.append(part)
        x = x - part.astype(F32)
    return parts


def kernel(
    n, table_hbm, mask_hbm, w_hbm, bias_hbm, out_ref,
    table_ref, mask_ref, bias_ref,
    tally, planes, prefix, raw, hold, came, joined, w_ref, wcat,
    send_sem, recv_sem, raw_send, raw_recv, count_send, count_recv, plane_send, plane_recv, load_sem,
):
    half, height = table_hbm.shape
    width = out_ref.shape[1]
    lines = height // 128
    levels = (n - 1).bit_length()
    lanes = height // CHUNKS
    side = min(PLANE, n)
    crowd = min(RAW, n)
    first = (crowd - 1).bit_length()
    count_planes = n // side
    me = lax.axis_index("rows")
    core = lax.axis_index("section")
    plane = me // side
    seat = lax.rem(me, side)

    columns = pl.ds(pl.multiple_of(core * width, 128), width)
    mask_copy = pltpu.make_async_copy(mask_hbm, mask_ref, load_sem.at[0])
    table_copy = pltpu.make_async_copy(table_hbm, table_ref, load_sem.at[1])
    w_copy = pltpu.make_async_copy(w_hbm.at[:, columns], w_ref, load_sem.at[2])
    bias_copy = pltpu.make_async_copy(bias_hbm.at[:, columns], bias_ref, load_sem.at[3])
    for load in (mask_copy, table_copy, w_copy, bias_copy):
        load.start()

    def seat_peer(step):
        return plane * side + lax.rem(seat + step, side)

    def plane_peer(step):
        return lax.rem(plane + step, count_planes) * side + seat

    barrier = pltpu.get_barrier_semaphore()
    for step in range(1, side):
        pl.semaphore_signal(barrier, inc=1, device_id={"rows": seat_peer(step)})
    for step in range(1, count_planes):
        pl.semaphore_signal(barrier, inc=1, device_id={"rows": plane_peer(step)})
    pl.semaphore_signal(barrier, inc=1, device_id={"section": 1 - core})

    mask_copy.wait()
    mask = mask_ref[...]
    ones = mask.astype(F32).astype(BF16)
    row = lax.broadcasted_iota(I32, (128, 128), 0)
    col = lax.broadcasted_iota(I32, (128, 128), 1)
    before = jnp.where(row < col, 1.0, 0.0).astype(BF16)
    inner = jnp.dot(ones, before, preferred_element_type=F32).astype(I32)
    sums = jnp.dot(ones, jnp.ones((128, 128), BF16), preferred_element_type=F32).astype(I32)
    running = jnp.zeros((1, 128), I32)
    starts = []
    for line in range(lines):
        starts.append(running)
        running = running + sums[line : line + 1]
    tally[seat] = running
    slot = jnp.where(mask == 1, inner + jnp.concatenate(starts, 0), -1)

    own = lax.rem(me, crowd)
    table_copy.wait()
    turned = jnp.concatenate(split(table_ref[...], 3), 0)
    for chunk in range(CHUNKS):
        here = chunk * lanes + lax.broadcasted_iota(I32, (lanes, 128), 0)
        hot = jnp.concatenate(
            [jnp.where(here == slot[b : b + 1], 1.0, 0.0).astype(BF16) for b in range(chunk * lanes // 128, lines)], 1
        )
        folded = lax.dot_general(
            turned[:, chunk * lanes :], hot, (((1,), (1,)), ((), ())), preferred_element_type=F32
        )
        raw[own, :, chunk * lanes : (chunk + 1) * lanes] = (
            folded[:half] + folded[half : 2 * half]
        ) + folded[2 * half :]

    pl.semaphore_wait(barrier, side + count_planes - 1)

    def seat_copy(step):
        return pltpu.make_async_remote_copy(
            src_ref=tally.at[seat], dst_ref=tally.at[seat],
            send_sem=count_send.at[step], recv_sem=count_recv.at[step],
            device_id={"rows": seat_peer(step)},
        )

    def plane_copy(step):
        return pltpu.make_async_remote_copy(
            src_ref=planes.at[plane], dst_ref=planes.at[plane],
            send_sem=plane_send.at[step], recv_sem=plane_recv.at[step],
            device_id={"rows": plane_peer(step)},
        )

    def raw_copy(step):
        return pltpu.make_async_remote_copy(
            src_ref=raw.at[own], dst_ref=raw.at[own],
            send_sem=raw_send.at[step], recv_sem=raw_recv.at[step],
            device_id={"rows": me - own + lax.rem(own + step, crowd)},
        )

    for step in range(1, side):
        seat_copy(step).start()
    for step in range(1, crowd):
        raw_copy(step).start()
    for step in range(1, side):
        seat_copy(step).wait_recv()
    everyone = jnp.zeros((1, 128), I32)
    for at in range(side):
        everyone = everyone + tally[at]
    planes[plane] = everyone
    for step in range(1, count_planes):
        plane_copy(step).start()

    w_copy.wait()
    bias_copy.wait()
    bias = bias_ref[...]
    w_hi, w_lo = split(w_ref[...], 2)
    b_hi, b_mid, b_lo = [part.astype(F32) for part in split(bias, 3)]
    line = lax.broadcasted_iota(I32, (16, width), 0)
    extra = jnp.where(line == 0, b_hi, jnp.where(line == 1, b_mid, jnp.where(line == 2, b_lo, 0.0)))
    wcat[...] = jnp.concatenate([w_hi, w_lo, w_hi, extra.astype(BF16)], 0)

    for step in range(1, count_planes):
        plane_copy(step).wait_recv()
    total = jnp.zeros((1, 128), I32)
    for at in range(count_planes):
        prefix[at * side] = total
        total = total + planes[at]
    prefix[n] = total
    running = prefix[plane * side]
    for at in range(side - 1):
        running = running + tally[at]
        prefix[plane * side + at + 1] = running

    def wide(x):
        return jnp.concatenate([x] * (lanes // 128), 1)

    def data_copy(level, chunk):
        at = (slice(None), pl.ds(chunk * lanes, lanes))
        return pltpu.make_async_remote_copy(
            src_ref=hold.at[(level,) + at], dst_ref=came.at[(level,) + at],
            send_sem=send_sem.at[level, chunk], recv_sem=recv_sem.at[level, chunk],
            device_id={"rows": me + (1 - 2 * (me // (1 << level) % 2)) * (1 << level)},
        )

    def join_copy(chunk):
        at = (core, slice(None), pl.ds(chunk * lanes, lanes))
        return pltpu.make_async_remote_copy(
            src_ref=joined.at[at], dst_ref=joined.at[at],
            send_sem=send_sem.at[levels, chunk], recv_sem=recv_sem.at[levels, chunk],
            device_id={"section": 1 - core},
        )

    for step in range(1, crowd):
        raw_copy(step).wait_recv()
    turns = []
    for at in range(crowd):
        shift = (prefix[me - own + at] & (height - 1))[0, 0]
        turns.append(pltpu.roll(raw[at], shift, 1))
    low = wide(prefix[me - own])
    for chunk in range(CHUNKS):
        at = slice(chunk * lanes, (chunk + 1) * lanes)
        base = own * height + chunk * lanes + lax.broadcasted_iota(I32, (1, lanes), 1)
        place = low + ((base - low) & (crowd * height - 1))
        place = jnp.broadcast_to(place, (half, lanes))
        block = turns[0][:, at]
        for other in range(1, crowd):
            block = jnp.where(place >= wide(prefix[me - own + other]), turns[other][:, at], block)
        hold[first, :, at] = block
        data_copy(first, chunk).start()

    for level in range(first, levels):
        reach = 2 << level
        group = me // reach * reach
        bit = me // (1 << level) % 2
        low = wide(prefix[group])
        middle = wide(prefix[group + (1 << level)])
        for chunk in range(CHUNKS):
            at = slice(chunk * lanes, (chunk + 1) * lanes)
            data_copy(level, chunk).wait_recv()
            base = (me % reach) * height + chunk * lanes
            base = base + lax.broadcasted_iota(I32, (1, lanes), 1)
            place = low + ((base - low) & (reach * height - 1))
            upper = jnp.where(place >= middle, 1, 0)
            foreign = jnp.broadcast_to(upper, (half, lanes)) != bit
            block = jnp.where(foreign, came[level, :, at], hold[level, :, at])
            if level < levels - 1:
                hold[level + 1, :, at] = block
                data_copy(level + 1, chunk).start()
            else:
                joined[core, :, at] = block
                join_copy(chunk).start()

    ends = wide(total)
    for chunk in range(CHUNKS):
        at = slice(chunk * lanes, (chunk + 1) * lanes)
        join_copy(chunk).wait_recv()
        owned = me * height + chunk * lanes + lax.broadcasted_iota(I32, (1, lanes), 1)
        filled = jnp.where(owned < ends, 1.0, 0.0)
        rows = jnp.concatenate([joined[0, :, at], joined[1, :, at]], 0)
        rows = jnp.where(jnp.broadcast_to(filled, rows.shape) > 0.5, rows, 0.0)
        a_hi, a_lo = split(rows, 2)
        marks = jnp.broadcast_to(filled, (16, lanes)).astype(BF16)
        lhs = jnp.concatenate([a_hi, a_hi, a_lo, marks], 0)
        out_ref[at, :] = lax.dot_general(
            lhs, wcat[...], (((0,), (0,)), ((), ())), preferred_element_type=F32
        ).astype(BF16)

    for step in range(1, side):
        seat_copy(step).wait_send()
    for step in range(1, count_planes):
        plane_copy(step).wait_send()
    for step in range(1, crowd):
        raw_copy(step).wait_send()
    for level in range(first, levels):
        for chunk in range(CHUNKS):
            data_copy(level, chunk).wait_send()
    for chunk in range(CHUNKS):
        join_copy(chunk).wait_send()


def solution(mesh):
    n, sections = mesh.shape["rows"], mesh.shape["section"]

    def step(table, mask, weight, bias):
        height, half = table.shape
        cols, features = weight.shape
        width = features // sections
        levels = (n - 1).bit_length()
        side, crowd = min(PLANE, n), min(RAW, n)
        operands = table.T, mask.reshape(height // 128, 128), weight, bias.reshape(1, features)
        vmem = pl.BlockSpec(memory_space=pltpu.VMEM)
        sem = pltpu.SemaphoreType.DMA
        return pl.pallas_call(
            functools.partial(kernel, n),
            name="filter_project",
            out_shape=jax.ShapeDtypeStruct((height, width), BF16),
            in_specs=[pl.BlockSpec(memory_space=pltpu.HBM)] * 4,
            out_specs=vmem,
            scratch_shapes=[
                pltpu.VMEM((half, height), F32),
                pltpu.VMEM((height // 128, 128), I32),
                pltpu.VMEM((1, width), F32),
                pltpu.VMEM((side, 1, 128), I32),
                pltpu.VMEM((n // side, 1, 128), I32),
                pltpu.VMEM((n + 1, 1, 128), I32),
                pltpu.VMEM((crowd, half, height), F32),
                pltpu.VMEM((levels, half, height), F32),
                pltpu.VMEM((levels, half, height), F32),
                pltpu.VMEM((sections, half, height), F32),
                pltpu.VMEM((cols, width), F32),
                pltpu.VMEM((3 * cols + 16, width), BF16),
                sem((levels + 1, CHUNKS)), sem((levels + 1, CHUNKS)),
                sem((crowd,)), sem((crowd,)),
                sem((side,)), sem((side,)),
                sem((n // side,)), sem((n // side,)),
                sem((4,)),
            ],
            compiler_params=pltpu.CompilerParams(
                collective_id=0, has_side_effects=True, vmem_limit_bytes=16 << 20
            ),
        )(*[pltpu.with_memory_space_constraint(x, pltpu.HBM) for x in operands])

    return jax.shard_map(
        step,
        mesh=mesh,
        in_specs=(P("rows", "section"), P("rows"), P(), P()),
        out_specs=P("rows", "section"),
        check_vma=False,
    )
```
